32 devices in a mesh: row: 4 (over z), col: 8 (over y, x, core).
Axes of the slice: x: 2, y: 2, z: 4, core: 2. Of those that a mesh axis runs over, the one named last changes fastest.
Arguments:
- a_matrix: float32 [8192, 8192], P('row', 'col'), may hold values from -14 to 30, as said below
- b_matrix: float32 [4096, 4096], P('row', 'col'), may hold values from -14 to 30, as said below
- c_matrix: float32 [8192, 4096], P('row', 'col'), may hold values from -6 to 6
Outputs:
- a_swept: float32 [8192, 8192], P('row', 'col')
- c_swept: float32 [8192, 4096], P('row', 'col')
- b_next: float32 [4096, 4096], P('row', 'col')
The draws below stay inside these ranges and needn't reach their ends.
Inputs may be any that keep to these rules, and one draw needn't show every extreme that they name: `a_matrix`: symmetric positive definite; its smallest eigenvalue is at least 1. `b_matrix`: symmetric positive definite; its smallest eigenvalue is at least 1.
All inputs are finite; a program needn't handle non-finite values. Where the reference program divides by a largest or mean magnitude, that divisor is 1e-20 or more.
Results may differ from the reference program's by a relative error of at most 0.00012.
Values sent between devices are 32-bit elements; how exact they have to be, the bound alone decides.
No kernel may reach another device: no remote copies, remote signals or barrier semaphores. Data moves between devices by JAX's collectives and lax.ppermute only.
A program may use at most 128 MiB of HBM per device.

```python
import math
import jax
import jax.numpy as jnp
from jax import lax

NA = 8192
NB = 4096
PANEL = 256
PIVOT_ITERS = 6
STEPS_A = 2
STEPS_B = 16


def definite(key, order):
    first_key, second_key, third_key = jax.random.split(key, 3)
    inner = order // 4
    limit = math.sqrt(3.0)
    factor = jax.random.uniform(first_key, (order, inner), jnp.float32, -limit, limit)
    spread = math.log(2.0)
    coupling = jnp.dot(factor, factor.T, precision=lax.Precision.HIGHEST, preferred_element_type=jnp.float32) / inner
    block_scale = jnp.exp(jax.random.uniform(second_key, (16,), jnp.float32, 0.0, 0.5 * spread))
    block_scale = jnp.repeat(block_scale, order // 16)
    row_scale = block_scale * jnp.exp(jax.random.uniform(third_key, (order,), jnp.float32, 0.0, 0.5 * spread))
    identity = jnp.eye(order, dtype=jnp.float32)
    core = identity + 0.25 * coupling
    return row_scale[:, None] * core * row_scale[None, :]


def draw_a_matrix(key, part):
    return definite(jax.random.fold_in(key, 11), NA)


def draw_b_matrix(key, part):
    return definite(jax.random.fold_in(key, 23), NB)


def steps_of(key, extent, cuts, low, high):
    loudness = 1.0
    for axis_at, shards_of in cuts:
        steps = jax.random.uniform(jax.random.fold_in(jax.random.fold_in(key, 6), axis_at), (shards_of,), jnp.float32, low / len(cuts), high / len(cuts))
        loudness = loudness * jnp.repeat(jnp.exp(steps), extent[axis_at] // shards_of).reshape((-1,) + (1,) * (len(extent) - 1 - axis_at))
    return loudness


def scatter_about(rng, extent, deviation, bound, pieces=(), held_as=jnp.bfloat16):
    gain = steps_of(rng, extent, pieces, -0.22, 0.18) if pieces else 1.0
    values = jax.random.normal(rng, extent, jnp.float32) * deviation * gain
    return jnp.minimum(jnp.maximum(values, -bound), bound).astype(held_as)


def setup_inputs(seed: int = 0) -> dict:
    keys = jax.random.split(jax.random.key(seed), 4)
    a_matrix = draw_a_matrix(jax.random.fold_in(keys[3], 71), 0)
    b_matrix = draw_b_matrix(jax.random.fold_in(keys[3], 71), 0)
    c_matrix = scatter_about(keys[2], (NA, NB), 1.0, 6.0, ((0, 4), (1, 8)), jnp.float32)
    return dict(a_matrix=a_matrix, b_matrix=b_matrix, c_matrix=c_matrix)


EXACT = lax.Precision.HIGHEST

def pivot_inverse(pivot):
    order = pivot.shape[0]
    scaling = 1.0 / jnp.sqrt(jnp.diagonal(pivot))
    unit = pivot * scaling[:, None] * scaling[None, :]
    ceiling = jnp.max(lax.optimization_barrier(jnp.sum(jnp.abs(unit), axis=1)))
    approx = jnp.eye(order, dtype=jnp.float32) / ceiling
    for turn in range(PIVOT_ITERS):
        product = jnp.dot(unit, approx, precision=EXACT, preferred_element_type=jnp.float32)
        approx = 2.0 * approx - jnp.dot(approx, product, precision=EXACT, preferred_element_type=jnp.float32)
    return approx * scaling[:, None] * scaling[None, :]

def sweep(matrix, other, count):
    order = matrix.shape[0]
    index = jnp.arange(order, dtype=jnp.int32)
    for step in range(count):
        first = step * PANEL
        eye_rows = (index[:, None] == first + jnp.arange(PANEL, dtype=jnp.int32)[None, :]).astype(jnp.float32)
        inverse = pivot_inverse(matrix[first:first + PANEL, first:first + PANEL])
        solved = jnp.dot(matrix[:, first:first + PANEL] - eye_rows, inverse, precision=EXACT, preferred_element_type=jnp.float32)
        rows = matrix[first:first + PANEL, :]
        updated = matrix - jnp.dot(solved, rows, precision=EXACT, preferred_element_type=jnp.float32)
        matrix = updated.at[:, first:first + PANEL].set(eye_rows - solved)
        if other is not None:
            other = other - jnp.dot(solved, other[first:first + PANEL, :], precision=EXACT, preferred_element_type=jnp.float32)
    return (matrix, other)

def reference(a_matrix, b_matrix, c_matrix):
    a_swept, c_swept = sweep(a_matrix, c_matrix, STEPS_A)
    b_inverse, unused = sweep(b_matrix, None, STEPS_B)
    b_squares = jnp.sum(b_matrix * b_matrix)
    inv_squares = jnp.sum(b_inverse * b_inverse)
    scale = jnp.sqrt(jnp.sqrt(inv_squares / b_squares))
    b_next = 0.5 * (scale * b_matrix + b_inverse / scale)
    return (a_swept, c_swept, b_next)
```

```python
import jax
import jax.numpy as jnp
from jax import lax
from jax.sharding import PartitionSpec as P

PANEL = 256
PIVOT_ITERS = 6
STEPS_A = 2
STEPS_B = 16


EXACT = lax.Precision.HIGHEST
CLOSE = lax.Precision.HIGH


def spread(value, axis, source):
    kept = jnp.where(lax.axis_index(axis) == source, value, 0).astype(value.dtype)
    return lax.psum(kept, axis)


def pivot_inverse(pivot):
    order = pivot.shape[0]
    unit_square = jnp.eye(order, dtype=jnp.float32)
    scaling = 1.0 / jnp.sqrt(jnp.sum(pivot * unit_square, axis=1))
    unit = pivot * scaling[:, None] * scaling[None, :]
    ceiling = jnp.max(jnp.sum(jnp.abs(unit), axis=1))
    approx = jnp.eye(order, dtype=jnp.float32) / ceiling
    for turn in range(PIVOT_ITERS):
        product = jnp.dot(unit, approx, precision=EXACT, preferred_element_type=jnp.float32)
        approx = 2.0 * approx - jnp.dot(
            approx, product, precision=EXACT, preferred_element_type=jnp.float32
        )
    return approx * scaling[:, None] * scaling[None, :]


def mul(left, right, dims, precision):
    return lax.dot_general(
        left, right, (dims, ((), ())), precision=precision, preferred_element_type=jnp.float32
    )


def sweep_panel(block, panel, places):
    order = block.shape[0]
    index = jnp.arange(order, dtype=jnp.int32)
    eye = (index[:, None] == jnp.concatenate([index, places])[None, :]).astype(jnp.float32)
    both = jnp.concatenate([block, panel], 1)
    for start in range(0, order, PANEL):
        stop = start + PANEL
        inverse = pivot_inverse(both[start:stop, start:stop].T)
        solved = mul(inverse, both[start:stop] - eye[start:stop], ((0,), (0,)), EXACT)
        updated = both - mul(both[:, start:stop], solved, ((1,), (0,)), CLOSE)
        both = jnp.concatenate(
            [updated[:start], eye[start:stop] - solved, updated[stop:]], 0
        )
    return both[:, order:], eye[:, order:]


def a_sweep(matrix, other):
    local_rows, local_cols = matrix.shape
    other_cols = other.shape[1]
    order = STEPS_A * PANEL
    row_place = lax.axis_index("row")
    col_place = lax.axis_index("col")
    panel = spread(matrix[:, :order], "col", 0)
    joined = spread(
        jnp.concatenate([matrix[:order], other[:order], panel[:order]], 1), "row", 0
    )
    rows = joined[:, : local_cols + other_cols]
    block = joined[:, local_cols + other_cols :].T
    places = row_place * local_rows + jnp.arange(local_rows, dtype=jnp.int32)
    swept, eye = sweep_panel(block, panel.T, places)
    solved = eye - swept
    new_matrix = matrix - mul(solved, rows[:, :local_cols], ((0,), (0,)), CLOSE)
    new_other = other - mul(solved, rows[:, local_cols:], ((0,), (0,)), CLOSE)
    front = jnp.where(col_place == 0, swept.T, new_matrix[:, :order])
    return new_matrix.at[:, :order].set(front), new_other


def b_sweep(matrix, row_count, col_count):
    local_rows, local_cols = matrix.shape
    order = min(local_rows, local_cols)
    steps = STEPS_B * PANEL // order
    row_part = order // row_count
    col_part = order // col_count
    row_place = lax.axis_index("row")
    col_place = lax.axis_index("col")
    dealt = matrix.T.reshape(local_cols // order, col_count, col_part, local_rows)
    dealt = lax.all_to_all(dealt, "col", 1, 0, tiled=True).reshape(local_cols, local_rows)
    dealt = dealt.T.reshape(local_rows // order, row_count, row_part, local_cols)
    dealt = lax.all_to_all(dealt, "row", 1, 0, tiled=True).reshape(local_rows, local_cols)
    index = jnp.arange(local_rows, dtype=jnp.int32)
    for step in range(steps):
        top = step * row_part
        left = step * col_part
        panel = lax.all_gather(dealt[:, left : left + col_part].T, "col", axis=0, tiled=True)
        joined = jnp.concatenate(
            [dealt[top : top + row_part], panel[:, top : top + row_part].T], 1
        )
        joined = lax.all_gather(joined, "row", axis=0, tiled=True)
        rows = joined[:, :local_cols]
        block = joined[:, local_cols:].T
        inside = (index >= top) & (index < top + row_part)
        places = jnp.where(inside, index - top + row_place * row_part, -1)
        swept, eye = sweep_panel(block, panel, places)
        updated = dealt + mul(swept - eye, rows, ((0,), (0,)), CLOSE)
        own = lax.dynamic_slice_in_dim(swept, col_place * col_part, col_part, 0).T
        dealt = updated.at[:, left : left + col_part].set(own)
    back = dealt.reshape(steps, 1, row_part, local_cols)
    back = lax.all_to_all(back, "row", 0, 1, tiled=True).reshape(local_rows, local_cols)
    back = back.T.reshape(steps, 1, col_part, local_rows)
    back = lax.all_to_all(back, "col", 0, 1, tiled=True).reshape(local_cols, local_rows)
    return back.T


def solution(mesh):
    row_count = mesh.shape["row"]
    col_count = mesh.shape["col"]

    def body(a_matrix, b_matrix, c_matrix):
        b_local = jnp.sum(b_matrix * b_matrix)
        a_swept, c_swept = a_sweep(a_matrix, c_matrix)
        b_inverse = b_sweep(b_matrix, row_count, col_count)
        inv_local = jnp.sum(b_inverse * b_inverse)
        sums = lax.psum(jnp.stack([b_local, inv_local]), ("row", "col"))
        scale = jnp.sqrt(jnp.sqrt(sums[1] / sums[0]))
        b_next = 0.5 * (scale * b_matrix + b_inverse / scale)
        return (a_swept, c_swept, b_next)

    return jax.shard_map(
        body,
        mesh=mesh,
        in_specs=(P("row", "col"), P("row", "col"), P("row", "col")),
        out_specs=(P("row", "col"), P("row", "col"), P("row", "col")),
        check_vma=False,
    )
```
